512 devices in a mesh: seq: 128 (over x, y, z_hi, core), ch: 4 (over z_lo).
Axes of the slice: x: 4, y: 4, z: 16 (z_hi: 4, z_lo: 4; z = z_hi * 4 + z_lo), core: 2. Of those that a mesh axis runs over, the one named last changes fastest.
Arguments:
- out_gate: bfloat16 [4096, 16384], P('ch', 'seq'), may hold values from -6 to 6
- key_proj: bfloat16 [4096, 16384], P('ch', 'seq'), may hold values from -6 to 6
- value_proj: bfloat16 [4096, 16384], P('ch', 'seq'), may hold values from -6 to 6
- long_filter: bfloat16 [4096, 16384], P('ch', 'seq'), may hold values from -0.046875 to 0.046875
- skip_gain: float32 [4096], P('ch'), may hold values from -4 to 4
- residual: bfloat16 [4096, 16384], P('ch', 'seq'), may hold values from -6 to 6
- norm_gain: float32 [4096], P('ch'), may hold values from 0.5 to 1.5
Outputs:
- mixed: bfloat16 [4096, 16384], P('ch', 'seq')
- normed: bfloat16 [4096, 16384], P('ch', 'seq')
The draws below stay inside these ranges and needn't reach their ends.
All inputs are finite; a program needn't handle non-finite values.
Results may differ from the reference program's by a relative error of at most 0.0075.
Values may be sent and summed in bfloat16 or wider, within the bound.
No kernel may reach another device: no remote copies, remote signals or barrier semaphores. Data moves between devices by JAX's collectives and lax.ppermute only.
A program may use at most 64 MiB of HBM per device.

```python
import jax
import jax.numpy as jnp
from jax import lax

D = 4096
SEQ = 16384


def block_levels(rng, extent, split, least, high):
    factor_of, own = 1.0, jax.random.fold_in(rng, 6)
    for position, shards_of in split:
        draws = jnp.exp(jax.random.uniform(jax.random.fold_in(own, position), (shards_of,), jnp.float32, least / len(split), high / len(split)))
        factor_of = factor_of * jnp.repeat(draws, extent[position] // shards_of).reshape([-1 if axis == position else 1 for axis in range(len(extent))])
    return factor_of


def centred(own_key, dims, width, limit, shards=(), kind=jnp.bfloat16):
    drawn = jax.random.normal(own_key, dims, jnp.float32) * width
    if len(shards) > 0:
        drawn = block_levels(own_key, dims, shards, -0.22, 0.18) * drawn
    return jnp.clip(drawn, min=-limit, max=limit).astype(kind)


def setup_inputs(seed: int = 0) -> dict:
    key_of = jax.random.split(jax.random.key(seed), 8)
    return {
        "out_gate": centred(key_of[0], (D, SEQ), 1.0, 6.0, ((0, 4), (1, 128))),
        "key_proj": centred(key_of[1], (D, SEQ), 1.0, 6.0, ((0, 4), (1, 128))),
        "value_proj": centred(key_of[2], (D, SEQ), 1.0, 6.0, ((0, 4), (1, 128))),
        "long_filter": centred(key_of[3], (D, SEQ), SEQ ** -0.5, 0.046875, ((0, 4), (1, 128))),
        "skip_gain": centred(key_of[4], (D,), 1.0, 4.0, ((0, 4),), jnp.float32),
        "residual": centred(key_of[5], (D, SEQ), 1.0, 6.0, ((0, 4), (1, 128))),
        "norm_gain": jnp.clip(1.0 + 0.1 * jax.random.normal(key_of[6], (D,), jnp.float32), 0.5, 1.5),
    }


def reference(out_gate, key_proj, value_proj, long_filter, skip_gain, residual, norm_gain):
    product_in = (key_proj.astype(jnp.float32) * value_proj.astype(jnp.float32)).astype(jnp.bfloat16)
    group_width = 64
    groups = D // group_width

    def one_group(pieces):
        signal, kernel, gate_rows, skip_rows, stream_rows = pieces
        signal_f = signal.astype(jnp.float32)
        length = signal_f.shape[1]
        spectrum = jnp.fft.rfft(signal_f, n=2 * length, axis=1) * jnp.fft.rfft(kernel.astype(jnp.float32), n=2 * length, axis=1)
        convolved = jnp.fft.irfft(spectrum, n=2 * length, axis=1)[:, :length].astype(signal_f.dtype)
        return stream_rows.astype(jnp.float32) + gate_rows.astype(jnp.float32) * (convolved + skip_rows[:, None] * signal_f)
    total = lax.map(one_group, (product_in.reshape(groups, group_width, -1), long_filter.reshape(groups, group_width, -1), out_gate.reshape(groups, group_width, -1), skip_gain.reshape(groups, group_width), residual.reshape(groups, group_width, -1)))
    total = total.reshape(D, -1)
    mixed = total.astype(jnp.bfloat16)
    mean_square = lax.optimization_barrier(jnp.mean(total * total, axis=0))
    normed = (total * lax.rsqrt(mean_square + 1e-06)[None, :] * norm_gain[:, None]).astype(jnp.bfloat16)
    return (mixed, normed)
```

```python
import math

import jax
import jax.numpy as jnp
import numpy as np
from jax import lax
from jax.experimental import pallas as pl
from jax.experimental.pallas import tpu as pltpu
from jax.sharding import PartitionSpec as P

D = 4096
BLOCKS = 128
WIDTH = 128
GROUP = 8
SPAN = 256

F32 = jnp.float32
BF16 = jnp.bfloat16


def split_table(table):
    high = table.astype(np.float32).astype(jnp.bfloat16)
    low = (table - high.astype(np.float64)).astype(np.float32).astype(jnp.bfloat16)
    return high, low


def angles(odd, plain):
    return ((2 * odd + 1) * plain % (2 * SPAN)).astype(np.float64) * (math.pi / SPAN)


def tables(arrival, departure):
    steps = np.arange(WIDTH)
    freqs = np.arange(WIDTH)
    phase = angles(freqs[None, :], steps[:, None])
    enter = np.concatenate([np.cos(phase), -np.sin(phase)], axis=1)
    enter_hi, enter_lo = split_table(enter)
    enter_both = np.concatenate([enter_hi, enter_lo], axis=0)

    phase = angles(freqs[:, None], arrival[None, :])
    over = np.concatenate([np.cos(phase), np.sin(phase)], axis=0)
    over_hi, over_lo = split_table(over)
    over_hi = np.concatenate([over_hi, over_hi], axis=1)
    over_lo = np.concatenate([over_lo, over_lo], axis=1)

    def back_rows(blocks):
        phase = angles(freqs[None, :], blocks[:, None])
        rows = np.concatenate([np.cos(phase), np.sin(phase)], axis=1) / SPAN
        return np.where(blocks[:, None] >= 0, rows, 0.0)

    back = np.concatenate([back_rows(departure), back_rows(departure - 1)], axis=0)
    back_hi, back_lo = split_table(back)

    def leave_rows(places):
        phase = angles(freqs[:, None], places[None, :])
        return np.concatenate([np.cos(phase), -np.sin(phase)], axis=0) * (2.0 / SPAN)

    leave = np.concatenate([leave_rows(steps), leave_rows(steps + WIDTH)], axis=0)
    leave_hi, leave_lo = split_table(leave)
    return enter_both, over_hi, over_lo, back_hi, back_lo, leave_hi, leave_lo


def dot(left, right):
    return jnp.dot(left, right, preferred_element_type=F32)


def halves(value):
    high = value.astype(BF16)
    return high, (value - high.astype(F32)).astype(BF16)


def convolve_kernel(
    rows_ref, enter_ref, over_hi_ref, over_lo_ref, back_hi_ref, back_lo_ref,
    leave_hi_ref, leave_lo_ref, out_ref, real_ref, imag_ref, time_ref,
):
    chunk = 256
    for start in range(0, 2 * GROUP * BLOCKS, chunk):
        piece = rows_ref[start : start + chunk, :]
        spectrum = dot(jnp.concatenate([piece, piece], axis=1), enter_ref[...])
        real_ref[start : start + chunk, :] = spectrum[:, :WIDTH]
        imag_ref[start : start + chunk, :] = spectrum[:, WIDTH:]

    def over_blocks(row):
        rows = pl.ds(row, BLOCKS, stride=2 * GROUP)
        high, low = halves(jnp.concatenate([real_ref[rows, :], imag_ref[rows, :]], axis=1))
        both = jnp.concatenate([high, low], axis=0)
        sums = dot(over_hi_ref[...], both) + dot(over_lo_ref[...], both)
        cos_re, cos_im = sums[:WIDTH, :WIDTH], sums[:WIDTH, WIDTH:]
        sin_re, sin_im = sums[WIDTH:, :WIDTH], sums[WIDTH:, WIDTH:]
        return cos_re + sin_im, cos_im - sin_re, cos_re - sin_im, cos_im + sin_re

    for chan in range(GROUP):
        xp_re, xp_im, xm_re, xm_im = over_blocks(chan)
        hp_re, hp_im, hm_re, hm_im = over_blocks(GROUP + chan)
        pp_re = xp_re * hp_re - xp_im * hp_im
        pp_im = xp_re * hp_im + xp_im * hp_re
        pm_re = xm_re * hm_re - xm_im * hm_im
        pm_im = xm_re * hm_im + xm_im * hm_re
        joint = jnp.concatenate(
            [
                jnp.concatenate([pp_re + pm_re, pp_im + pm_im], axis=1),
                jnp.concatenate([pm_im - pp_im, pp_re - pm_re], axis=1),
            ],
            axis=0,
        )
        joint_hi, joint_lo = halves(joint)
        blocks = (
            dot(back_hi_ref[...], joint_hi)
            + dot(back_hi_ref[...], joint_lo)
            + dot(back_lo_ref[...], joint_hi)
        )
        pair_hi, pair_lo = halves(
            jnp.concatenate([blocks[:BLOCKS, :], blocks[BLOCKS:, :]], axis=1)
        )
        time_ref[pl.ds(chan, BLOCKS, stride=GROUP), :] = (
            dot(pair_hi, leave_hi_ref[...])
            + dot(pair_lo, leave_hi_ref[...])
            + dot(pair_hi, leave_lo_ref[...])
        )
    out_ref[...] = time_ref[...].astype(BF16)


def convolve(rows, consts, interpret=False):
    return pl.pallas_call(
        convolve_kernel,
        out_shape=jax.ShapeDtypeStruct((GROUP * BLOCKS, WIDTH), BF16),
        scratch_shapes=[
            pltpu.VMEM((2 * GROUP * BLOCKS, WIDTH), F32),
            pltpu.VMEM((2 * GROUP * BLOCKS, WIDTH), F32),
            pltpu.VMEM((GROUP * BLOCKS, WIDTH), F32),
        ],
        name="convolve",
        interpret=interpret,
    )(rows, *consts)


def on_device(out_gate, key_proj, value_proj, long_filter, skip_gain, residual, norm_gain):
    chans, width = key_proj.shape
    blocks = lax.axis_size("seq")
    order = np.arange(blocks)
    consts = [jnp.asarray(table) for table in tables(order, order)]
    gated = lax.reduce_precision(key_proj.astype(F32) * value_proj.astype(F32), 8, 7)
    both = jnp.concatenate(
        [gated.astype(BF16).reshape(blocks, GROUP, width), long_filter.reshape(blocks, GROUP, width)],
        axis=1,
    )
    arrived = lax.all_to_all(both, "seq", 0, 0, tiled=True)
    convolved = convolve(arrived.reshape(2 * GROUP * blocks, width), consts)
    convolved = lax.all_to_all(convolved.reshape(blocks, GROUP, width), "seq", 0, 0, tiled=True)
    convolved = convolved.reshape(chans, width).astype(F32)
    total = residual.astype(F32) + out_gate.astype(F32) * (convolved + skip_gain[:, None] * gated)
    squares = jnp.sum(total * total, axis=0, keepdims=True)
    count = lax.axis_size("ch")
    squares = jnp.sum(
        lax.all_to_all(
            jnp.broadcast_to(squares[None], (count, 1, width)), "ch", 0, 0, tiled=True
        ),
        axis=0,
    )
    normed = total * lax.rsqrt(squares / D + 1e-06) * norm_gain[:, None]
    return (total.astype(BF16), normed.astype(BF16))


def solution(mesh):
    return jax.shard_map(
        on_device,
        mesh=mesh,
        in_specs=(
            P("ch", "seq"),
            P("ch", "seq"),
            P("ch", "seq"),
            P("ch", "seq"),
            P("ch"),
            P("ch", "seq"),
            P("ch"),
        ),
        out_specs=(P("ch", "seq"), P("ch", "seq")),
        check_vma=False,
    )
```

```python
import math

import jax
import jax.numpy as jnp
import numpy as np
from jax import lax
from jax.experimental import pallas as pl
from jax.experimental.pallas import tpu as pltpu
from jax.sharding import PartitionSpec as P

D = 4096
BLOCKS = 128
WIDTH = 128
GROUP = 8
SPAN = 256

F32 = jnp.float32
BF16 = jnp.bfloat16


def split_table(table):
    high = table.astype(np.float32).astype(jnp.bfloat16)
    low = (table - high.astype(np.float64)).astype(np.float32).astype(jnp.bfloat16)
    return high, low


def angles(odd, plain):
    return ((2 * odd + 1) * plain % (2 * SPAN)).astype(np.float64) * (math.pi / SPAN)


def tables():
    steps = np.arange(WIDTH)
    phase = angles(steps[None, :], steps[:, None])
    enter = np.concatenate([np.cos(phase), -np.sin(phase)], axis=1)
    enter = np.concatenate(split_table(enter), axis=0)

    phase = angles(steps[:, None], steps[None, :])
    over = np.concatenate([np.cos(phase), np.sin(phase)], axis=0)
    over_hi, over_lo = (np.concatenate([part, part], axis=1) for part in split_table(over))

    phase = angles(steps[None, :], steps[:, None])
    back = np.concatenate([np.cos(phase), np.sin(phase)], axis=1) / SPAN
    back = np.concatenate(split_table(back), axis=0)

    phase = angles(steps[:, None], np.arange(SPAN)[None, :])
    leave = np.concatenate([np.cos(phase), -np.sin(phase)], axis=0) * (2.0 / SPAN)
    leave_hi, leave_lo = split_table(leave)
    return enter, over_hi, over_lo, back, leave_hi, leave_lo


def dot(left, right):
    return jnp.dot(left, right, preferred_element_type=F32)


def halves(value):
    high = value.astype(BF16)
    return high, (value - high.astype(F32)).astype(BF16)


def convolve_kernel(
    rows_ref, enter_ref, over_hi_ref, over_lo_ref, back_ref, leave_hi_ref, leave_lo_ref,
    out_ref, real_ref, imag_ref, joint_hi_ref, joint_lo_ref, pair_hi_ref, pair_lo_ref,
    early_ref, late_ref,
):
    chunk = 256
    for start in range(0, 2 * GROUP * BLOCKS, chunk):
        piece = rows_ref[start : start + chunk, :]
        spectrum = dot(jnp.concatenate([piece, piece], axis=1), enter_ref[...])
        real_ref[start : start + chunk, :] = spectrum[:, :WIDTH]
        imag_ref[start : start + chunk, :] = spectrum[:, WIDTH:]

    def over_blocks(row):
        rows = pl.ds(row, BLOCKS, stride=2 * GROUP)
        high, low = halves(jnp.concatenate([real_ref[rows, :], imag_ref[rows, :]], axis=1))
        both = jnp.concatenate([high, low], axis=0)
        sums = dot(over_hi_ref[...], both) + dot(over_lo_ref[...], both)
        cos_re, cos_im = sums[:WIDTH, :WIDTH], sums[:WIDTH, WIDTH:]
        sin_re, sin_im = sums[WIDTH:, :WIDTH], sums[WIDTH:, WIDTH:]
        return cos_re + sin_im, cos_im - sin_re, cos_re - sin_im, cos_im + sin_re

    for chan in range(GROUP):
        xp_re, xp_im, xm_re, xm_im = over_blocks(chan)
        hp_re, hp_im, hm_re, hm_im = over_blocks(GROUP + chan)
        pp_re = xp_re * hp_re - xp_im * hp_im
        pp_im = xp_re * hp_im + xp_im * hp_re
        pm_re = xm_re * hm_re - xm_im * hm_im
        pm_im = xm_re * hm_im + xm_im * hm_re
        quarters = (pp_re + pm_re, pp_im + pm_im, pm_im - pp_im, pp_re - pm_re)
        for place, quarter in enumerate(quarters):
            rows = pl.ds((2 * chan + place // 2) * WIDTH, WIDTH)
            lanes = pl.ds(place % 2 * WIDTH, WIDTH)
            joint_hi_ref[rows, lanes], joint_lo_ref[rows, lanes] = halves(quarter)

    for chan in range(GROUP):
        joint = pl.ds(chan * SPAN, SPAN)
        rows = pl.ds(chan * BLOCKS, BLOCKS)
        sums = dot(back_ref[...], joint_hi_ref[joint, :])
        low = dot(back_ref[:BLOCKS, :], joint_lo_ref[joint, :])
        pair_hi_ref[rows, :], pair_lo_ref[rows, :] = halves(sums[:BLOCKS] + sums[BLOCKS:] + low)

    late_ref[pl.ds(0, GROUP), :] = jnp.zeros((GROUP, WIDTH), F32)
    for chan in range(GROUP):
        rows = pl.ds(chan * BLOCKS, BLOCKS)
        high, low = pair_hi_ref[rows, :], pair_lo_ref[rows, :]
        timeline = (
            dot(high, leave_hi_ref[...])
            + dot(low, leave_hi_ref[...])
            + dot(high, leave_lo_ref[...])
        )
        early_ref[pl.ds(chan, BLOCKS, stride=GROUP), :] = timeline[:, :WIDTH]
        late_ref[pl.ds(GROUP + chan, BLOCKS, stride=GROUP), :] = timeline[:, WIDTH:]
    out_ref[...] = (early_ref[...] + late_ref[: GROUP * BLOCKS, :]).astype(BF16)


def in_vmem(value):
    return pltpu.with_memory_space_constraint(value, pltpu.VMEM)


def convolve(rows, consts):
    return pl.pallas_call(
        convolve_kernel,
        out_shape=pltpu.VMEM((GROUP * BLOCKS, WIDTH), BF16),
        scratch_shapes=[
            pltpu.VMEM((2 * GROUP * BLOCKS, WIDTH), F32),
            pltpu.VMEM((2 * GROUP * BLOCKS, WIDTH), F32),
            pltpu.VMEM((GROUP * SPAN, SPAN), BF16),
            pltpu.VMEM((GROUP * SPAN, SPAN), BF16),
            pltpu.VMEM((GROUP * BLOCKS, SPAN), BF16),
            pltpu.VMEM((GROUP * BLOCKS, SPAN), BF16),
            pltpu.VMEM((GROUP * BLOCKS, WIDTH), F32),
            pltpu.VMEM((GROUP * (BLOCKS + 1), WIDTH), F32),
        ],
        name="convolve",
    )(in_vmem(rows), *[in_vmem(table) for table in consts])


def on_device(out_gate, key_proj, value_proj, long_filter, skip_gain, residual, norm_gain):
    chans, width = key_proj.shape
    blocks = lax.axis_size("seq")
    consts = [jnp.asarray(table) for table in tables()]
    gated = lax.reduce_precision(key_proj.astype(F32) * value_proj.astype(F32), 8, 7)
    both = jnp.concatenate(
        [gated.astype(BF16).reshape(blocks, GROUP, width), long_filter.reshape(blocks, GROUP, width)],
        axis=1,
    )
    arrived = lax.all_to_all(both, "seq", 0, 0, tiled=True)
    convolved = convolve(arrived.reshape(2 * GROUP * blocks, width), consts)
    convolved = lax.all_to_all(convolved.reshape(blocks, GROUP, width), "seq", 0, 0, tiled=True)
    convolved = convolved.reshape(chans, width).astype(F32)
    total = residual.astype(F32) + out_gate.astype(F32) * (convolved + skip_gain[:, None] * gated)
    mixed, scaled, squares = lax.optimization_barrier(
        (
            total.astype(BF16),
            total * norm_gain[:, None],
            jnp.sum(total * total, axis=0, keepdims=True),
        )
    )
    count = lax.axis_size("ch")
    squares = jnp.sum(
        lax.all_to_all(
            jnp.broadcast_to(squares[None], (count, 1, width)), "ch", 0, 0, tiled=True
        ),
        axis=0,
    )
    normed = scaled * lax.rsqrt(squares / D + 1e-06)
    return (mixed, normed.astype(BF16))


def solution(mesh):
    return jax.shard_map(
        on_device,
        mesh=mesh,
        in_specs=(
            P("ch", "seq"),
            P("ch", "seq"),
            P("ch", "seq"),
            P("ch", "seq"),
            P("ch"),
            P("ch", "seq"),
            P("ch"),
        ),
        out_specs=(P("ch", "seq"), P("ch", "seq")),
        check_vma=False,
    )
```

```python
import math

import jax
import jax.numpy as jnp
import numpy as np
from jax import lax
from jax.experimental import pallas as pl
from jax.experimental.pallas import tpu as pltpu
from jax.sharding import PartitionSpec as P

D = 4096
BLOCKS = 128
WIDTH = 128
GROUP = 8
SPAN = 256

F32 = jnp.float32
BF16 = jnp.bfloat16


def split_table(table):
    high = table.astype(np.float32).astype(jnp.bfloat16)
    low = (table - high.astype(np.float64)).astype(np.float32).astype(jnp.bfloat16)
    return high, low


def angles(odd, plain):
    return ((2 * odd + 1) * plain % (2 * SPAN)).astype(np.float64) * (math.pi / SPAN)


def tables():
    steps = np.arange(WIDTH)
    phase = angles(steps[None, :], steps[:, None])
    enter = np.concatenate([np.cos(phase), -np.sin(phase)], axis=1)
    enter = np.concatenate(split_table(enter), axis=0)

    phase = angles(steps[:, None], steps[None, :])
    over = np.concatenate([np.cos(phase), np.sin(phase)], axis=0)
    over_hi, over_lo = (np.concatenate([part, part], axis=1) for part in split_table(over))

    phase = angles(steps[None, :], steps[:, None])
    back = np.concatenate([np.cos(phase), np.sin(phase)], axis=1) / SPAN
    back = np.concatenate(split_table(back), axis=0)

    phase = angles(steps[:, None], np.arange(SPAN)[None, :])
    leave = np.concatenate([np.cos(phase), -np.sin(phase)], axis=0) * (2.0 / SPAN)
    leave_hi, leave_lo = split_table(leave)
    return enter, over_hi, over_lo, back, leave_hi, leave_lo


def dot(left, right):
    return jnp.dot(left, right, preferred_element_type=F32)


def halves(value):
    high = value.astype(BF16)
    return high, (value - high.astype(F32)).astype(BF16)


def convolve_kernel(
    rows_ref, gain_ref, enter_ref, over_hi_ref, over_lo_ref, back_ref, leave_hi_ref,
    leave_lo_ref, out_ref, kept_ref, real_ref, imag_ref, joint_hi_ref, joint_lo_ref, pair_hi_ref, pair_lo_ref,
    early_ref, late_ref,
):
    chunk = 256
    for start in range(0, 2 * GROUP * BLOCKS, chunk):
        piece = rows_ref[start : start + chunk, :]
        spectrum = dot(jnp.concatenate([piece, piece], axis=1), enter_ref[...])
        real_ref[start : start + chunk, :] = spectrum[:, :WIDTH]
        imag_ref[start : start + chunk, :] = spectrum[:, WIDTH:]

    def over_blocks(row):
        rows = pl.ds(row, BLOCKS, stride=2 * GROUP)
        high, low = halves(jnp.concatenate([real_ref[rows, :], imag_ref[rows, :]], axis=1))
        both = jnp.concatenate([high, low], axis=0)
        sums = dot(over_hi_ref[...], both) + dot(over_lo_ref[...], both)
        cos_re, cos_im = sums[:WIDTH, :WIDTH], sums[:WIDTH, WIDTH:]
        sin_re, sin_im = sums[WIDTH:, :WIDTH], sums[WIDTH:, WIDTH:]
        return cos_re + sin_im, cos_im - sin_re, cos_re - sin_im, cos_im + sin_re

    for chan in range(GROUP):
        xp_re, xp_im, xm_re, xm_im = over_blocks(chan)
        hp_re, hp_im, hm_re, hm_im = over_blocks(GROUP + chan)
        pp_re = xp_re * hp_re - xp_im * hp_im
        pp_im = xp_re * hp_im + xp_im * hp_re
        pm_re = xm_re * hm_re - xm_im * hm_im
        pm_im = xm_re * hm_im + xm_im * hm_re
        quarters = (pp_re + pm_re, pp_im + pm_im, pm_im - pp_im, pp_re - pm_re)
        for place, quarter in enumerate(quarters):
            rows = pl.ds((2 * chan + place // 2) * WIDTH, WIDTH)
            lanes = pl.ds(place % 2 * WIDTH, WIDTH)
            joint_hi_ref[rows, lanes], joint_lo_ref[rows, lanes] = halves(quarter)

    for chan in range(GROUP):
        joint = pl.ds(chan * SPAN, SPAN)
        rows = pl.ds(chan * BLOCKS, BLOCKS)
        sums = dot(back_ref[...], joint_hi_ref[joint, :])
        low = dot(back_ref[:BLOCKS, :], joint_lo_ref[joint, :])
        pair_hi_ref[rows, :], pair_lo_ref[rows, :] = halves(sums[:BLOCKS] + sums[BLOCKS:] + low)

    late_ref[pl.ds(0, GROUP), :] = jnp.zeros((GROUP, WIDTH), F32)
    for chan in range(GROUP):
        rows = pl.ds(chan * BLOCKS, BLOCKS)
        high, low = pair_hi_ref[rows, :], pair_lo_ref[rows, :]
        timeline = (
            dot(high, leave_hi_ref[...])
            + dot(low, leave_hi_ref[...])
            + dot(high, leave_lo_ref[...])
        )
        early_ref[pl.ds(chan, BLOCKS, stride=GROUP), :] = timeline[:, :WIDTH]
        late_ref[pl.ds(GROUP + chan, BLOCKS, stride=GROUP), :] = timeline[:, WIDTH:]
    kept_ref[...] = gain_ref[...]
    out_ref[...] = (early_ref[...] + late_ref[: GROUP * BLOCKS, :]).astype(BF16)


def in_vmem(value):
    return pltpu.with_memory_space_constraint(value, pltpu.VMEM)


def convolve(rows, gain, consts):
    return pl.pallas_call(
        convolve_kernel,
        out_shape=(
            pltpu.VMEM((GROUP * BLOCKS, WIDTH), BF16),
            pltpu.VMEM(gain.shape, F32),
        ),
        scratch_shapes=[
            pltpu.VMEM((2 * GROUP * BLOCKS, WIDTH), F32),
            pltpu.VMEM((2 * GROUP * BLOCKS, WIDTH), F32),
            pltpu.VMEM((GROUP * SPAN, SPAN), BF16),
            pltpu.VMEM((GROUP * SPAN, SPAN), BF16),
            pltpu.VMEM((GROUP * BLOCKS, SPAN), BF16),
            pltpu.VMEM((GROUP * BLOCKS, SPAN), BF16),
            pltpu.VMEM((GROUP * BLOCKS, WIDTH), F32),
            pltpu.VMEM((GROUP * (BLOCKS + 1), WIDTH), F32),
        ],
        name="convolve",
    )(in_vmem(rows), in_vmem(gain), *[in_vmem(table) for table in consts])


def on_device(out_gate, key_proj, value_proj, long_filter, skip_gain, residual, norm_gain):
    chans, width = key_proj.shape
    blocks = lax.axis_size("seq")
    consts = [jnp.asarray(table) for table in tables()]
    gated = lax.reduce_precision(key_proj.astype(F32) * value_proj.astype(F32), 8, 7)
    both = jnp.concatenate(
        [gated.astype(BF16).reshape(blocks, GROUP, width), long_filter.reshape(blocks, GROUP, width)],
        axis=1,
    )
    arrived = lax.all_to_all(both, "seq", 0, 0, tiled=True)
    convolved, gain = convolve(
        arrived.reshape(2 * GROUP * blocks, width),
        norm_gain.reshape(chans // WIDTH, WIDTH),
        consts,
    )
    convolved = lax.all_to_all(convolved.reshape(blocks, GROUP, width), "seq", 0, 0, tiled=True)
    convolved = convolved.reshape(chans, width).astype(F32)
    total = residual.astype(F32) + out_gate.astype(F32) * (convolved + skip_gain[:, None] * gated)
    squares = jnp.sum(total * total, axis=0, keepdims=True)
    count = lax.axis_size("ch")
    squares = jnp.sum(
        lax.all_to_all(
            jnp.broadcast_to(squares[None], (count, 1, width)), "ch", 0, 0, tiled=True
        ),
        axis=0,
    )
    normed = total * lax.rsqrt(squares / D + 1e-06) * gain.reshape(chans)[:, None]
    return (total.astype(BF16), normed.astype(BF16))


def solution(mesh):
    return jax.shard_map(
        on_device,
        mesh=mesh,
        in_specs=(
            P("ch", "seq"),
            P("ch", "seq"),
            P("ch", "seq"),
            P("ch", "seq"),
            P("ch"),
            P("ch", "seq"),
            P("ch"),
        ),
        out_specs=(P("ch", "seq"), P("ch", "seq")),
        check_vma=False,
    )
```

```python
import math

import jax
import jax.numpy as jnp
import numpy as np
from jax import lax
from jax.experimental import pallas as pl
from jax.experimental.pallas import tpu as pltpu
from jax.sharding import Mesh
from jax.sharding import PartitionSpec as P

D = 4096
BLOCKS = 128
WIDTH = 128
GROUP = 8
SPAN = 256

F32 = jnp.float32
BF16 = jnp.bfloat16


def split_table(table):
    high = table.astype(np.float32).astype(jnp.bfloat16)
    low = (table - high.astype(np.float64)).astype(np.float32).astype(jnp.bfloat16)
    return high, low


def angles(odd, plain):
    return ((2 * odd + 1) * plain % (2 * SPAN)).astype(np.float64) * (math.pi / SPAN)


def tables():
    steps = np.arange(WIDTH)
    phase = angles(steps[None, :], steps[:, None])
    enter = np.concatenate([np.cos(phase), -np.sin(phase)], axis=1)
    enter = np.concatenate(split_table(enter), axis=0)

    phase = angles(steps[:, None], steps[None, :])
    over = np.concatenate([np.cos(phase), np.sin(phase)], axis=0)
    over_hi, over_lo = (np.concatenate([part, part], axis=1) for part in split_table(over))

    phase = angles(steps[None, :], steps[:, None])
    back = np.concatenate([np.cos(phase), np.sin(phase)], axis=1) / SPAN
    back = np.concatenate(split_table(back), axis=0)

    phase = angles(steps[:, None], np.arange(SPAN)[None, :])
    leave = np.concatenate([np.cos(phase), -np.sin(phase)], axis=0) * (2.0 / SPAN)
    leave_hi, leave_lo = split_table(leave)
    return enter, over_hi, over_lo, back, leave_hi, leave_lo


def dot(left, right):
    return jnp.dot(left, right, preferred_element_type=F32)


def halves(value):
    high = value.astype(BF16)
    return high, (value - high.astype(F32)).astype(BF16)


def convolve_kernel(
    core_ref, rows_ref, gain_ref, enter_ref, over_hi_ref, over_lo_ref, back_ref, leave_hi_ref,
    leave_lo_ref, own_ref, other_ref, kept_ref, real_ref, imag_ref, joint_hi_ref, joint_lo_ref, pair_hi_ref, pair_lo_ref,
    early_ref, late_ref,
):
    chunk = 256
    for start in range(0, 2 * GROUP * BLOCKS, chunk):
        piece = rows_ref[start : start + chunk, :]
        spectrum = dot(jnp.concatenate([piece, piece], axis=1), enter_ref[...])
        real_ref[start : start + chunk, :] = spectrum[:, :WIDTH]
        imag_ref[start : start + chunk, :] = spectrum[:, WIDTH:]

    def over_blocks(row):
        rows = pl.ds(row, BLOCKS, stride=2 * GROUP)
        high, low = halves(jnp.concatenate([real_ref[rows, :], imag_ref[rows, :]], axis=1))
        both = jnp.concatenate([high, low], axis=0)
        sums = dot(over_hi_ref[...], both) + dot(over_lo_ref[...], both)
        cos_re, cos_im = sums[:WIDTH, :WIDTH], sums[:WIDTH, WIDTH:]
        sin_re, sin_im = sums[WIDTH:, :WIDTH], sums[WIDTH:, WIDTH:]
        return cos_re + sin_im, cos_im - sin_re, cos_re - sin_im, cos_im + sin_re

    for chan in range(GROUP):
        xp_re, xp_im, xm_re, xm_im = over_blocks(chan)
        hp_re, hp_im, hm_re, hm_im = over_blocks(GROUP + chan)
        pp_re = xp_re * hp_re - xp_im * hp_im
        pp_im = xp_re * hp_im + xp_im * hp_re
        pm_re = xm_re * hm_re - xm_im * hm_im
        pm_im = xm_re * hm_im + xm_im * hm_re
        quarters = (pp_re + pm_re, pp_im + pm_im, pm_im - pp_im, pp_re - pm_re)
        for place, quarter in enumerate(quarters):
            rows = pl.ds((2 * chan + place // 2) * WIDTH, WIDTH)
            lanes = pl.ds(place % 2 * WIDTH, WIDTH)
            joint_hi_ref[rows, lanes], joint_lo_ref[rows, lanes] = halves(quarter)

    for chan in range(GROUP):
        joint = pl.ds(chan * SPAN, SPAN)
        rows = pl.ds(chan * BLOCKS, BLOCKS)
        sums = dot(back_ref[...], joint_hi_ref[joint, :])
        low = dot(back_ref[:BLOCKS, :], joint_lo_ref[joint, :])
        pair_hi_ref[rows, :], pair_lo_ref[rows, :] = halves(sums[:BLOCKS] + sums[BLOCKS:] + low)

    late_ref[pl.ds(0, GROUP), :] = jnp.zeros((GROUP, WIDTH), F32)
    for chan in range(GROUP):
        rows = pl.ds(chan * BLOCKS, BLOCKS)
        high, low = pair_hi_ref[rows, :], pair_lo_ref[rows, :]
        timeline = (
            dot(high, leave_hi_ref[...])
            + dot(low, leave_hi_ref[...])
            + dot(high, leave_lo_ref[...])
        )
        early_ref[pl.ds(chan, BLOCKS, stride=GROUP), :] = timeline[:, :WIDTH]
        late_ref[pl.ds(GROUP + chan, BLOCKS, stride=GROUP), :] = timeline[:, WIDTH:]
    kept_ref[...] = gain_ref[...]
    summed = (early_ref[...] + late_ref[: GROUP * BLOCKS, :]).reshape(
        BLOCKS // 2, 2 * GROUP, WIDTH
    )
    even, odd = summed[:, :GROUP].astype(BF16), summed[:, GROUP:].astype(BF16)

    @pl.when(core_ref[0] == 0)
    def _():
        own_ref[...] = even
        other_ref[...] = odd

    @pl.when(core_ref[0] != 0)
    def _():
        own_ref[...] = odd
        other_ref[...] = even


def in_vmem(value):
    return pltpu.with_memory_space_constraint(value, pltpu.VMEM)


def convolve(core, rows, gain, consts):
    return pl.pallas_call(
        convolve_kernel,
        in_specs=[pl.BlockSpec(memory_space=pltpu.SMEM)]
        + [pl.BlockSpec(memory_space=pltpu.VMEM)] * (2 + len(consts)),
        out_shape=(
            pltpu.VMEM((BLOCKS // 2, GROUP, WIDTH), BF16),
            pltpu.VMEM((BLOCKS // 2, GROUP, WIDTH), BF16),
            pltpu.VMEM(gain.shape, F32),
        ),
        scratch_shapes=[
            pltpu.VMEM((2 * GROUP * BLOCKS, WIDTH), F32),
            pltpu.VMEM((2 * GROUP * BLOCKS, WIDTH), F32),
            pltpu.VMEM((GROUP * SPAN, SPAN), BF16),
            pltpu.VMEM((GROUP * SPAN, SPAN), BF16),
            pltpu.VMEM((GROUP * BLOCKS, SPAN), BF16),
            pltpu.VMEM((GROUP * BLOCKS, SPAN), BF16),
            pltpu.VMEM((GROUP * BLOCKS, WIDTH), F32),
            pltpu.VMEM((GROUP * (BLOCKS + 1), WIDTH), F32),
        ],
        name="convolve",
    )(core, in_vmem(rows), in_vmem(gain), *[in_vmem(table) for table in consts])


def on_device(out_gate, key_proj, value_proj, long_filter, skip_gain, residual, norm_gain):
    chans, width = key_proj.shape
    blocks = lax.axis_size("chip") * lax.axis_size("core")
    core = lax.axis_index("core")
    consts = [jnp.asarray(table) for table in tables()]
    gated = lax.reduce_precision(key_proj.astype(F32) * value_proj.astype(F32), 8, 7)
    both = jnp.concatenate(
        [gated.astype(BF16).reshape(blocks, GROUP, width), long_filter.reshape(blocks, GROUP, width)],
        axis=1,
    )
    both, core = lax.optimization_barrier((both, core.astype(jnp.int32).reshape(1)))
    arrived = lax.all_to_all(both, ("chip", "core"), 0, 0, tiled=True)
    own, other, gain = convolve(
        core,
        arrived.reshape(2 * GROUP * blocks, width),
        norm_gain.reshape(chans // WIDTH, WIDTH),
        consts,
    )
    met = lax.ppermute(other, "core", [(0, 1), (1, 0)])
    both = jnp.where(
        core[0] == 0, jnp.concatenate([own, met], axis=1), jnp.concatenate([met, own], axis=1)
    )
    convolved = lax.all_to_all(both, "chip", 0, 0, tiled=True).reshape(chans, width).astype(F32)
    total = residual.astype(F32) + out_gate.astype(F32) * (convolved + skip_gain[:, None] * gated)
    squares = jnp.sum(total * total, axis=0, keepdims=True)
    count = lax.axis_size("ch")
    squares = jnp.sum(
        lax.all_to_all(
            jnp.broadcast_to(squares[None], (count, 1, width)), "ch", 0, 0, tiled=True
        ),
        axis=0,
    )
    normed = total * lax.rsqrt(squares / D + 1e-06) * gain.reshape(chans)[:, None]
    return (total.astype(BF16), normed.astype(BF16))


def solution(mesh):
    mesh = Mesh(mesh.devices.reshape(BLOCKS // 2, 2, -1), ("chip", "core", "ch"))
    wide, column = P("ch", ("chip", "core")), P("ch")
    return jax.shard_map(
        on_device,
        mesh=mesh,
        in_specs=(wide, wide, wide, wide, column, wide, column),
        out_specs=(wide, wide),
        check_vma=False,
    )
```

```python
import math

import jax
import jax.numpy as jnp
import numpy as np
from jax import lax
from jax.experimental import pallas as pl
from jax.experimental.pallas import tpu as pltpu
from jax.sharding import PartitionSpec as P

D = 4096
BLOCKS = 128
WIDTH = 128
GROUP = 8
SPAN = 256

F32 = jnp.float32
BF16 = jnp.bfloat16


def split_table(table):
    high = table.astype(np.float32).astype(jnp.bfloat16)
    low = (table - high.astype(np.float64)).astype(np.float32).astype(jnp.bfloat16)
    return high, low


def angles(odd, plain):
    return ((2 * odd + 1) * plain % (2 * SPAN)).astype(np.float64) * (math.pi / SPAN)


def tables():
    steps = np.arange(WIDTH)
    phase = angles(steps[None, :], steps[:, None])
    enter = np.concatenate([np.cos(phase), -np.sin(phase)], axis=1)
    enter = np.concatenate(split_table(enter), axis=0)

    phase = angles(steps[:, None], steps[None, :])
    over = np.concatenate([np.cos(phase), np.sin(phase)], axis=0)
    over_hi, over_lo = (np.concatenate([part, part], axis=1) for part in split_table(over))

    phase = angles(steps[None, :], steps[:, None])
    back = np.concatenate([np.cos(phase), np.sin(phase)], axis=1) / SPAN
    back = np.concatenate(split_table(back), axis=0)

    phase = angles(steps[:, None], np.arange(SPAN)[None, :])
    leave = np.concatenate([np.cos(phase), -np.sin(phase)], axis=0) * (2.0 / SPAN)
    leave_hi, leave_lo = split_table(leave)
    return enter, over_hi, over_lo, back, leave_hi, leave_lo


def dot(left, right):
    return jnp.dot(left, right, preferred_element_type=F32)


def halves(value):
    high = value.astype(BF16)
    return high, (value - high.astype(F32)).astype(BF16)


def convolve_kernel(
    rows_ref, gain_ref, enter_ref, over_hi_ref, over_lo_ref, back_ref, leave_hi_ref,
    leave_lo_ref, out_ref, kept_ref, in_re_ref, in_im_ref, lag_re_ref, lag_im_ref,
    joint_hi_ref, joint_lo_ref, pair_hi_ref, pair_lo_ref,
    early_ref, late_ref,
):
    chunk = 512
    for start in range(0, 2 * GROUP * BLOCKS, chunk):
        piece = rows_ref[start : start + chunk, :]
        spectrum = dot(jnp.concatenate([piece, piece], axis=1), enter_ref[...])
        spectrum = spectrum.reshape(chunk // (2 * GROUP), 2 * GROUP, SPAN)
        signal = spectrum[:, :GROUP].reshape(chunk // 2, SPAN)
        lags = spectrum[:, GROUP:].reshape(chunk // 2, SPAN)
        rows = pl.ds(start // 2, chunk // 2)
        in_re_ref[rows, :] = signal[:, :WIDTH]
        in_im_ref[rows, :] = signal[:, WIDTH:]
        lag_re_ref[rows, :] = lags[:, :WIDTH]
        lag_im_ref[rows, :] = lags[:, WIDTH:]

    def over_blocks(real_ref, imag_ref, chan):
        rows = pl.ds(chan, BLOCKS, stride=GROUP)
        high, low = halves(jnp.concatenate([real_ref[rows, :], imag_ref[rows, :]], axis=1))
        both = jnp.concatenate([high, low], axis=0)
        sums = dot(over_hi_ref[...], both) + dot(over_lo_ref[...], both)
        cos_re, cos_im = sums[:WIDTH, :WIDTH], sums[:WIDTH, WIDTH:]
        sin_re, sin_im = sums[WIDTH:, :WIDTH], sums[WIDTH:, WIDTH:]
        return cos_re + sin_im, cos_im - sin_re, cos_re - sin_im, cos_im + sin_re

    for chan in range(GROUP):
        xp_re, xp_im, xm_re, xm_im = over_blocks(in_re_ref, in_im_ref, chan)
        hp_re, hp_im, hm_re, hm_im = over_blocks(lag_re_ref, lag_im_ref, chan)
        pp_re = xp_re * hp_re - xp_im * hp_im
        pp_im = xp_re * hp_im + xp_im * hp_re
        pm_re = xm_re * hm_re - xm_im * hm_im
        pm_im = xm_re * hm_im + xm_im * hm_re
        quarters = (pp_re + pm_re, pp_im + pm_im, pm_im - pp_im, pp_re - pm_re)
        for place, quarter in enumerate(quarters):
            rows = pl.ds((2 * chan + place // 2) * WIDTH, WIDTH)
            lanes = pl.ds(place % 2 * WIDTH, WIDTH)
            joint_hi_ref[rows, lanes], joint_lo_ref[rows, lanes] = halves(quarter)

    for chan in range(GROUP):
        joint = pl.ds(chan * SPAN, SPAN)
        rows = pl.ds(chan * BLOCKS, BLOCKS)
        sums = dot(back_ref[...], joint_hi_ref[joint, :])
        low = dot(back_ref[:BLOCKS, :], joint_lo_ref[joint, :])
        pair_hi_ref[rows, :], pair_lo_ref[rows, :] = halves(sums[:BLOCKS] + sums[BLOCKS:] + low)

    late_ref[pl.ds(0, GROUP), :] = jnp.zeros((GROUP, WIDTH), F32)
    for chan in range(GROUP):
        rows = pl.ds(chan * BLOCKS, BLOCKS)
        high, low = pair_hi_ref[rows, :], pair_lo_ref[rows, :]
        timeline = (
            dot(high, leave_hi_ref[...])
            + dot(low, leave_hi_ref[...])
            + dot(high, leave_lo_ref[...])
        )
        early_ref[pl.ds(chan, BLOCKS, stride=GROUP), :] = timeline[:, :WIDTH]
        late_ref[pl.ds(GROUP + chan, BLOCKS, stride=GROUP), :] = timeline[:, WIDTH:]
    kept_ref[...] = gain_ref[...]
    out_ref[...] = (early_ref[...] + late_ref[: GROUP * BLOCKS, :]).astype(BF16)


def in_vmem(value):
    return pltpu.with_memory_space_constraint(value, pltpu.VMEM)


def convolve(rows, gain, consts):
    return pl.pallas_call(
        convolve_kernel,
        out_shape=(
            pltpu.VMEM((GROUP * BLOCKS, WIDTH), BF16),
            pltpu.VMEM(gain.shape, F32),
        ),
        scratch_shapes=[
            pltpu.VMEM((GROUP * BLOCKS, WIDTH), F32),
            pltpu.VMEM((GROUP * BLOCKS, WIDTH), F32),
            pltpu.VMEM((GROUP * BLOCKS, WIDTH), F32),
            pltpu.VMEM((GROUP * BLOCKS, WIDTH), F32),
            pltpu.VMEM((GROUP * SPAN, SPAN), BF16),
            pltpu.VMEM((GROUP * SPAN, SPAN), BF16),
            pltpu.VMEM((GROUP * BLOCKS, SPAN), BF16),
            pltpu.VMEM((GROUP * BLOCKS, SPAN), BF16),
            pltpu.VMEM((GROUP * BLOCKS, WIDTH), F32),
            pltpu.VMEM((GROUP * (BLOCKS + 1), WIDTH), F32),
        ],
        name="convolve",
    )(in_vmem(rows), in_vmem(gain), *[in_vmem(table) for table in consts])


def on_device(out_gate, key_proj, value_proj, long_filter, skip_gain, residual, norm_gain):
    chans, width = key_proj.shape
    blocks = lax.axis_size("seq")
    consts = [jnp.asarray(table) for table in tables()]
    gated = lax.reduce_precision(key_proj.astype(F32) * value_proj.astype(F32), 8, 7)
    both = jnp.concatenate(
        [gated.astype(BF16).reshape(blocks, GROUP, width), long_filter.reshape(blocks, GROUP, width)],
        axis=1,
    )
    arrived = lax.all_to_all(both, "seq", 0, 0, tiled=True)
    convolved, gain = convolve(
        arrived.reshape(2 * GROUP * blocks, width),
        norm_gain.reshape(chans // WIDTH, WIDTH),
        consts,
    )
    convolved = lax.all_to_all(convolved.reshape(blocks, GROUP, width), "seq", 0, 0, tiled=True)
    convolved = convolved.reshape(chans, width).astype(F32)
    total = residual.astype(F32) + out_gate.astype(F32) * (convolved + skip_gain[:, None] * gated)
    squares = jnp.sum(total * total, axis=0, keepdims=True)
    squares = jnp.sum(lax.all_gather(squares, "ch"), axis=0)
    normed = total * lax.rsqrt(squares / D + 1e-06) * gain.reshape(chans)[:, None]
    return (total.astype(BF16), normed.astype(BF16))


def solution(mesh):
    return jax.shard_map(
        on_device,
        mesh=mesh,
        in_specs=(
            P("ch", "seq"),
            P("ch", "seq"),
            P("ch", "seq"),
            P("ch", "seq"),
            P("ch"),
            P("ch", "seq"),
            P("ch"),
        ),
        out_specs=(P("ch", "seq"), P("ch", "seq")),
        check_vma=False,
    )
```

```python
import math

import jax
import jax.numpy as jnp
import numpy as np
from jax import lax
from jax.experimental import pallas as pl
from jax.experimental.pallas import tpu as pltpu
from jax.sharding import PartitionSpec as P

D = 4096
BLOCKS = 128
WIDTH = 128
GROUP = 8
LEAD = 85
CH_LEAD = 1
SPAN = 256

F32 = jnp.float32
BF16 = jnp.bfloat16


def led_by(first, count):
    order = list(range(count))
    order[0], order[first] = first, 0
    return order


def split_table(table):
    high = table.astype(np.float32).astype(jnp.bfloat16)
    low = (table - high.astype(np.float64)).astype(np.float32).astype(jnp.bfloat16)
    return high, low


def angles(odd, plain):
    return ((2 * odd + 1) * plain % (2 * SPAN)).astype(np.float64) * (math.pi / SPAN)


def tables():
    steps = np.arange(WIDTH)
    phase = angles(steps[None, :], steps[:, None])
    enter = np.concatenate([np.cos(phase), -np.sin(phase)], axis=1)
    enter = np.concatenate(split_table(enter), axis=0)

    arrival = np.array(led_by(LEAD, BLOCKS))
    phase = angles(steps[:, None], arrival[None, :])
    over = np.concatenate([np.cos(phase), np.sin(phase)], axis=0)
    over_hi, over_lo = (np.concatenate([part, part], axis=1) for part in split_table(over))

    phase = angles(steps[None, :], steps[:, None])
    back = np.concatenate([np.cos(phase), np.sin(phase)], axis=1) / SPAN
    back = np.concatenate(split_table(back), axis=0)

    phase = angles(steps[:, None], np.arange(SPAN)[None, :])
    leave = np.concatenate([np.cos(phase), -np.sin(phase)], axis=0) * (2.0 / SPAN)
    leave_hi, leave_lo = split_table(leave)
    return enter, over_hi, over_lo, back, leave_hi, leave_lo


def dot(left, right):
    return jnp.dot(left, right, preferred_element_type=F32)


def halves(value):
    high = value.astype(BF16)
    return high, (value - high.astype(F32)).astype(BF16)


def convolve_kernel(
    rows_ref, gain_ref, enter_ref, over_hi_ref, over_lo_ref, back_ref, leave_hi_ref,
    leave_lo_ref, out_ref, kept_ref, in_re_ref, in_im_ref, lag_re_ref, lag_im_ref,
    joint_hi_ref, joint_lo_ref, pair_hi_ref, pair_lo_ref,
    early_ref, late_ref,
):
    chunk = 512
    for start in range(0, 2 * GROUP * BLOCKS, chunk):
        piece = rows_ref[start : start + chunk, :]
        spectrum = dot(jnp.concatenate([piece, piece], axis=1), enter_ref[...])
        spectrum = spectrum.reshape(chunk // (2 * GROUP), 2 * GROUP, SPAN)
        signal = spectrum[:, :GROUP].reshape(chunk // 2, SPAN)
        lags = spectrum[:, GROUP:].reshape(chunk // 2, SPAN)
        rows = pl.ds(start // 2, chunk // 2)
        in_re_ref[rows, :] = signal[:, :WIDTH]
        in_im_ref[rows, :] = signal[:, WIDTH:]
        lag_re_ref[rows, :] = lags[:, :WIDTH]
        lag_im_ref[rows, :] = lags[:, WIDTH:]

    def over_blocks(real_ref, imag_ref, chan):
        rows = pl.ds(chan, BLOCKS, stride=GROUP)
        high, low = halves(jnp.concatenate([real_ref[rows, :], imag_ref[rows, :]], axis=1))
        both = jnp.concatenate([high, low], axis=0)
        sums = dot(over_hi_ref[...], both) + dot(over_lo_ref[...], both)
        cos_re, cos_im = sums[:WIDTH, :WIDTH], sums[:WIDTH, WIDTH:]
        sin_re, sin_im = sums[WIDTH:, :WIDTH], sums[WIDTH:, WIDTH:]
        return cos_re + sin_im, cos_im - sin_re, cos_re - sin_im, cos_im + sin_re

    for chan in range(GROUP):
        xp_re, xp_im, xm_re, xm_im = over_blocks(in_re_ref, in_im_ref, chan)
        hp_re, hp_im, hm_re, hm_im = over_blocks(lag_re_ref, lag_im_ref, chan)
        pp_re = xp_re * hp_re - xp_im * hp_im
        pp_im = xp_re * hp_im + xp_im * hp_re
        pm_re = xm_re * hm_re - xm_im * hm_im
        pm_im = xm_re * hm_im + xm_im * hm_re
        quarters = (pp_re + pm_re, pp_im + pm_im, pm_im - pp_im, pp_re - pm_re)
        for place, quarter in enumerate(quarters):
            rows = pl.ds((2 * chan + place // 2) * WIDTH, WIDTH)
            lanes = pl.ds(place % 2 * WIDTH, WIDTH)
            joint_hi_ref[rows, lanes], joint_lo_ref[rows, lanes] = halves(quarter)

    for chan in range(GROUP):
        joint = pl.ds(chan * SPAN, SPAN)
        rows = pl.ds(chan * BLOCKS, BLOCKS)
        sums = dot(back_ref[...], joint_hi_ref[joint, :])
        low = dot(back_ref[:BLOCKS, :], joint_lo_ref[joint, :])
        pair_hi_ref[rows, :], pair_lo_ref[rows, :] = halves(sums[:BLOCKS] + sums[BLOCKS:] + low)

    late_ref[pl.ds(0, GROUP), :] = jnp.zeros((GROUP, WIDTH), F32)
    for chan in range(GROUP):
        rows = pl.ds(chan * BLOCKS, BLOCKS)
        high, low = pair_hi_ref[rows, :], pair_lo_ref[rows, :]
        timeline = (
            dot(high, leave_hi_ref[...])
            + dot(low, leave_hi_ref[...])
            + dot(high, leave_lo_ref[...])
        )
        early_ref[pl.ds(chan, BLOCKS, stride=GROUP), :] = timeline[:, :WIDTH]
        late_ref[pl.ds(GROUP + chan, BLOCKS, stride=GROUP), :] = timeline[:, WIDTH:]
    kept_ref[...] = gain_ref[...]
    summed = early_ref[...] + late_ref[: GROUP * BLOCKS, :]
    lead = LEAD * GROUP
    out_ref[...] = jnp.concatenate(
        [
            summed[lead : lead + GROUP],
            summed[GROUP:lead],
            summed[:GROUP],
            summed[lead + GROUP :],
        ],
        axis=0,
    ).astype(BF16)


def in_vmem(value):
    return pltpu.with_memory_space_constraint(value, pltpu.VMEM)


def convolve(rows, gain, consts):
    return pl.pallas_call(
        convolve_kernel,
        out_shape=(
            pltpu.VMEM((GROUP * BLOCKS, WIDTH), BF16),
            pltpu.VMEM(gain.shape, F32),
        ),
        scratch_shapes=[
            pltpu.VMEM((GROUP * BLOCKS, WIDTH), F32),
            pltpu.VMEM((GROUP * BLOCKS, WIDTH), F32),
            pltpu.VMEM((GROUP * BLOCKS, WIDTH), F32),
            pltpu.VMEM((GROUP * BLOCKS, WIDTH), F32),
            pltpu.VMEM((GROUP * SPAN, SPAN), BF16),
            pltpu.VMEM((GROUP * SPAN, SPAN), BF16),
            pltpu.VMEM((GROUP * BLOCKS, SPAN), BF16),
            pltpu.VMEM((GROUP * BLOCKS, SPAN), BF16),
            pltpu.VMEM((GROUP * BLOCKS, WIDTH), F32),
            pltpu.VMEM((GROUP * (BLOCKS + 1), WIDTH), F32),
        ],
        name="convolve",
    )(in_vmem(rows), in_vmem(gain), *[in_vmem(table) for table in consts])


def on_device(out_gate, key_proj, value_proj, long_filter, skip_gain, residual, norm_gain):
    chans, width = key_proj.shape
    blocks = lax.axis_size("seq")
    consts = [jnp.asarray(table) for table in tables()]
    gated = lax.reduce_precision(key_proj.astype(F32) * value_proj.astype(F32), 8, 7)
    both = jnp.concatenate(
        [gated.astype(BF16).reshape(blocks, GROUP, width), long_filter.reshape(blocks, GROUP, width)],
        axis=1,
    )
    members = [led_by(LEAD, blocks)]
    arrived = lax.all_to_all(both, "seq", 0, 0, axis_index_groups=members, tiled=True)
    convolved, gain = convolve(
        arrived.reshape(2 * GROUP * blocks, width),
        norm_gain.reshape(chans // WIDTH, WIDTH),
        consts,
    )
    convolved = lax.all_to_all(
        convolved.reshape(blocks, GROUP, width),
        "seq",
        0,
        0,
        axis_index_groups=members,
        tiled=True,
    )
    convolved = convolved.reshape(chans, width).astype(F32)
    total = residual.astype(F32) + out_gate.astype(F32) * (convolved + skip_gain[:, None] * gated)
    squares = jnp.sum(total * total, axis=0, keepdims=True)
    owners = [led_by(CH_LEAD, lax.axis_size("ch"))]
    squares = jnp.sum(lax.all_gather(squares, "ch", axis_index_groups=owners), axis=0)
    normed = total * lax.rsqrt(squares / D + 1e-06) * gain.reshape(chans)[:, None]
    return (total.astype(BF16), normed.astype(BF16))


def solution(mesh):
    return jax.shard_map(
        on_device,
        mesh=mesh,
        in_specs=(
            P("ch", "seq"),
            P("ch", "seq"),
            P("ch", "seq"),
            P("ch", "seq"),
            P("ch"),
            P("ch", "seq"),
            P("ch"),
        ),
        out_specs=(P("ch", "seq"), P("ch", "seq")),
        check_vma=False,
    )
```

```python
import math

import jax
import jax.numpy as jnp
import numpy as np
from jax import lax
from jax.experimental import pallas as pl
from jax.experimental.pallas import tpu as pltpu
from jax.sharding import PartitionSpec as P

D = 4096
BLOCKS = 128
WIDTH = 128
GROUP = 8
LEAD = 85
CH_LEAD = 2
SPAN = 256

F32 = jnp.float32
BF16 = jnp.bfloat16


def led_by(first, count):
    order = list(range(count))
    order[0], order[first] = first, 0
    return order


def split_table(table):
    high = table.astype(np.float32).astype(jnp.bfloat16)
    low = (table - high.astype(np.float64)).astype(np.float32).astype(jnp.bfloat16)
    return high, low


def angles(odd, plain):
    return ((2 * odd + 1) * plain % (2 * SPAN)).astype(np.float64) * (math.pi / SPAN)


def tables():
    steps = np.arange(WIDTH)
    phase = angles(steps[None, :], steps[:, None])
    enter = np.concatenate([np.cos(phase), -np.sin(phase)], axis=1)
    enter = np.concatenate(split_table(enter), axis=0)

    arrival = np.array(led_by(LEAD, BLOCKS))
    phase = angles(steps[:, None], arrival[None, :])
    over = np.concatenate([np.cos(phase), np.sin(phase)], axis=0)
    over_hi, over_lo = (np.concatenate([part, part], axis=1) for part in split_table(over))

    phase = angles(steps[None, :], steps[:, None])
    back = np.concatenate([np.cos(phase), np.sin(phase)], axis=1) / SPAN
    back = np.concatenate(split_table(back), axis=0)

    phase = angles(steps[:, None], np.arange(SPAN)[None, :])
    leave = np.concatenate([np.cos(phase), -np.sin(phase)], axis=0) * (2.0 / SPAN)
    leave_hi, leave_lo = split_table(leave)
    return enter, over_hi, over_lo, back, leave_hi, leave_lo


def dot(left, right):
    return jnp.dot(left, right, preferred_element_type=F32)


def halves(value):
    high = value.astype(BF16)
    return high, (value - high.astype(F32)).astype(BF16)


def convolve_kernel(
    rows_ref, gain_ref, enter_ref, over_hi_ref, over_lo_ref, back_ref, leave_hi_ref,
    leave_lo_ref, out_ref, kept_ref, in_re_ref, in_im_ref, lag_re_ref, lag_im_ref,
    joint_hi_ref, joint_lo_ref, pair_hi_ref, pair_lo_ref,
    early_ref, late_ref,
):
    chunk = 512
    for start in range(0, 2 * GROUP * BLOCKS, chunk):
        piece = rows_ref[start : start + chunk, :]
        spectrum = dot(jnp.concatenate([piece, piece], axis=1), enter_ref[...])
        spectrum = spectrum.reshape(chunk // (2 * GROUP), 2 * GROUP, SPAN)
        signal = spectrum[:, :GROUP].reshape(chunk // 2, SPAN)
        lags = spectrum[:, GROUP:].reshape(chunk // 2, SPAN)
        rows = pl.ds(start // 2, chunk // 2)
        in_re_ref[rows, :] = signal[:, :WIDTH]
        in_im_ref[rows, :] = signal[:, WIDTH:]
        lag_re_ref[rows, :] = lags[:, :WIDTH]
        lag_im_ref[rows, :] = lags[:, WIDTH:]

    def over_blocks(real_ref, imag_ref, chan):
        rows = pl.ds(chan, BLOCKS, stride=GROUP)
        high, low = halves(jnp.concatenate([real_ref[rows, :], imag_ref[rows, :]], axis=1))
        both = jnp.concatenate([high, low], axis=0)
        sums = dot(over_hi_ref[...], both) + dot(over_lo_ref[...], both)
        cos_re, cos_im = sums[:WIDTH, :WIDTH], sums[:WIDTH, WIDTH:]
        sin_re, sin_im = sums[WIDTH:, :WIDTH], sums[WIDTH:, WIDTH:]
        return cos_re + sin_im, cos_im - sin_re, cos_re - sin_im, cos_im + sin_re

    for chan in range(GROUP):
        xp_re, xp_im, xm_re, xm_im = over_blocks(in_re_ref, in_im_ref, chan)
        hp_re, hp_im, hm_re, hm_im = over_blocks(lag_re_ref, lag_im_ref, chan)
        pp_re = xp_re * hp_re - xp_im * hp_im
        pp_im = xp_re * hp_im + xp_im * hp_re
        pm_re = xm_re * hm_re - xm_im * hm_im
        pm_im = xm_re * hm_im + xm_im * hm_re
        quarters = (pp_re + pm_re, pp_im + pm_im, pm_im - pp_im, pp_re - pm_re)
        for place, quarter in enumerate(quarters):
            rows = pl.ds((2 * chan + place // 2) * WIDTH, WIDTH)
            lanes = pl.ds(place % 2 * WIDTH, WIDTH)
            joint_hi_ref[rows, lanes], joint_lo_ref[rows, lanes] = halves(quarter)

    for chan in range(GROUP):
        joint = pl.ds(chan * SPAN, SPAN)
        rows = pl.ds(chan * BLOCKS, BLOCKS)
        sums = dot(back_ref[...], joint_hi_ref[joint, :])
        low = dot(back_ref[:BLOCKS, :], joint_lo_ref[joint, :])
        pair_hi_ref[rows, :], pair_lo_ref[rows, :] = halves(sums[:BLOCKS] + sums[BLOCKS:] + low)

    late_ref[pl.ds(0, GROUP), :] = jnp.zeros((GROUP, WIDTH), F32)
    for chan in range(GROUP):
        rows = pl.ds(chan * BLOCKS, BLOCKS)
        high, low = pair_hi_ref[rows, :], pair_lo_ref[rows, :]
        timeline = (
            dot(high, leave_hi_ref[...])
            + dot(low, leave_hi_ref[...])
            + dot(high, leave_lo_ref[...])
        )
        early_ref[pl.ds(chan, BLOCKS, stride=GROUP), :] = timeline[:, :WIDTH]
        late_ref[pl.ds(GROUP + chan, BLOCKS, stride=GROUP), :] = timeline[:, WIDTH:]
    kept_ref[...] = gain_ref[...]
    summed = early_ref[...] + late_ref[: GROUP * BLOCKS, :]
    lead = LEAD * GROUP
    out_ref[...] = jnp.concatenate(
        [
            summed[lead : lead + GROUP],
            summed[GROUP:lead],
            summed[:GROUP],
            summed[lead + GROUP :],
        ],
        axis=0,
    ).astype(BF16)


def in_vmem(value):
    return pltpu.with_memory_space_constraint(value, pltpu.VMEM)


def convolve(rows, gain, consts):
    return pl.pallas_call(
        convolve_kernel,
        out_shape=(
            pltpu.VMEM((GROUP * BLOCKS, WIDTH), BF16),
            pltpu.VMEM(gain.shape, F32),
        ),
        scratch_shapes=[
            pltpu.VMEM((GROUP * BLOCKS, WIDTH), F32),
            pltpu.VMEM((GROUP * BLOCKS, WIDTH), F32),
            pltpu.VMEM((GROUP * BLOCKS, WIDTH), F32),
            pltpu.VMEM((GROUP * BLOCKS, WIDTH), F32),
            pltpu.VMEM((GROUP * SPAN, SPAN), BF16),
            pltpu.VMEM((GROUP * SPAN, SPAN), BF16),
            pltpu.VMEM((GROUP * BLOCKS, SPAN), BF16),
            pltpu.VMEM((GROUP * BLOCKS, SPAN), BF16),
            pltpu.VMEM((GROUP * BLOCKS, WIDTH), F32),
            pltpu.VMEM((GROUP * (BLOCKS + 1), WIDTH), F32),
        ],
        name="convolve",
    )(in_vmem(rows), in_vmem(gain), *[in_vmem(table) for table in consts])


def on_device(out_gate, key_proj, value_proj, long_filter, skip_gain, residual, norm_gain):
    chans, width = key_proj.shape
    blocks = lax.axis_size("seq")
    consts = [jnp.asarray(table) for table in tables()]
    gated = lax.reduce_precision(key_proj.astype(F32) * value_proj.astype(F32), 8, 7)
    both = jnp.concatenate(
        [gated.astype(BF16).reshape(blocks, GROUP, width), long_filter.reshape(blocks, GROUP, width)],
        axis=1,
    )
    members = [led_by(LEAD, blocks)]
    arrived = lax.all_to_all(both, "seq", 0, 0, axis_index_groups=members, tiled=True)
    convolved, gain = convolve(
        arrived.reshape(2 * GROUP * blocks, width),
        norm_gain.reshape(chans // WIDTH, WIDTH),
        consts,
    )
    convolved = lax.all_to_all(
        convolved.reshape(blocks, GROUP, width),
        "seq",
        0,
        0,
        axis_index_groups=members,
        tiled=True,
    )
    convolved = convolved.reshape(chans, width).astype(F32)
    total = residual.astype(F32) + out_gate.astype(F32) * (convolved + skip_gain[:, None] * gated)
    squares = jnp.sum(total * total, axis=0, keepdims=True)
    count = lax.axis_size("ch")
    squares = jnp.sum(
        lax.all_to_all(
            jnp.broadcast_to(squares[None], (count, 1, width)),
            "ch",
            0,
            0,
            axis_index_groups=[led_by(CH_LEAD, count)],
            tiled=True,
        ),
        axis=0,
    )
    normed = total * lax.rsqrt(squares / D + 1e-06) * gain.reshape(chans)[:, None]
    return (total.astype(BF16), normed.astype(BF16))


def solution(mesh):
    return jax.shard_map(
        on_device,
        mesh=mesh,
        in_specs=(
            P("ch", "seq"),
            P("ch", "seq"),
            P("ch", "seq"),
            P("ch", "seq"),
            P("ch"),
            P("ch", "seq"),
            P("ch"),
        ),
        out_specs=(P("ch", "seq"), P("ch", "seq")),
        check_vma=False,
    )
```

```python
import math

import jax
import jax.numpy as jnp
import numpy as np
from jax import lax
from jax.experimental import pallas as pl
from jax.experimental.pallas import tpu as pltpu
from jax.sharding import PartitionSpec as P

D = 4096
BLOCKS = 128
WIDTH = 128
GROUP = 8
LEAD = 93
CH_LEAD = 2
SPAN = 256

F32 = jnp.float32
BF16 = jnp.bfloat16


def led_by(first, count):
    order = list(range(count))
    order[0], order[first] = first, 0
    return order


def split_table(table):
    high = table.astype(np.float32).astype(jnp.bfloat16)
    low = (table - high.astype(np.float64)).astype(np.float32).astype(jnp.bfloat16)
    return high, low


def angles(odd, plain):
    return ((2 * odd + 1) * plain % (2 * SPAN)).astype(np.float64) * (math.pi / SPAN)


def tables():
    steps = np.arange(WIDTH)
    phase = angles(steps[None, :], steps[:, None])
    enter = np.concatenate([np.cos(phase), -np.sin(phase)], axis=1)
    enter = np.concatenate(split_table(enter), axis=0)

    arrival = np.array(led_by(LEAD, BLOCKS))
    phase = angles(steps[:, None], arrival[None, :])
    over = np.concatenate([np.cos(phase), np.sin(phase)], axis=0)
    over_hi, over_lo = (np.concatenate([part, part], axis=1) for part in split_table(over))

    phase = angles(steps[None, :], steps[:, None])
    back = np.concatenate([np.cos(phase), np.sin(phase)], axis=1) / SPAN
    back = np.concatenate(split_table(back), axis=0)

    phase = angles(steps[:, None], np.arange(SPAN)[None, :])
    leave = np.concatenate([np.cos(phase), -np.sin(phase)], axis=0) * (2.0 / SPAN)
    leave_hi, leave_lo = split_table(leave)
    return enter, over_hi, over_lo, back, leave_hi, leave_lo


def dot(left, right):
    return jnp.dot(left, right, preferred_element_type=F32)


def halves(value):
    high = value.astype(BF16)
    return high, (value - high.astype(F32)).astype(BF16)


def convolve_kernel(
    rows_ref, gain_ref, enter_ref, over_hi_ref, over_lo_ref, back_ref, leave_hi_ref,
    leave_lo_ref, out_ref, kept_ref, in_re_ref, in_im_ref, lag_re_ref, lag_im_ref,
    joint_hi_ref, joint_lo_ref, pair_hi_ref, pair_lo_ref,
    early_ref, late_ref,
):
    chunk = 512
    for start in range(0, 2 * GROUP * BLOCKS, chunk):
        piece = rows_ref[start : start + chunk, :]
        spectrum = dot(jnp.concatenate([piece, piece], axis=1), enter_ref[...])
        spectrum = spectrum.reshape(chunk // (2 * GROUP), 2 * GROUP, SPAN)
        signal = spectrum[:, :GROUP].reshape(chunk // 2, SPAN)
        lags = spectrum[:, GROUP:].reshape(chunk // 2, SPAN)
        rows = pl.ds(start // 2, chunk // 2)
        in_re_ref[rows, :] = signal[:, :WIDTH]
        in_im_ref[rows, :] = signal[:, WIDTH:]
        lag_re_ref[rows, :] = lags[:, :WIDTH]
        lag_im_ref[rows, :] = lags[:, WIDTH:]

    def over_blocks(real_ref, imag_ref, chan):
        rows = pl.ds(chan, BLOCKS, stride=GROUP)
        high, low = halves(jnp.concatenate([real_ref[rows, :], imag_ref[rows, :]], axis=1))
        both = jnp.concatenate([high, low], axis=0)
        sums = dot(over_hi_ref[...], both) + dot(over_lo_ref[...], both)
        cos_re, cos_im = sums[:WIDTH, :WIDTH], sums[:WIDTH, WIDTH:]
        sin_re, sin_im = sums[WIDTH:, :WIDTH], sums[WIDTH:, WIDTH:]
        return cos_re + sin_im, cos_im - sin_re, cos_re - sin_im, cos_im + sin_re

    for chan in range(GROUP):
        xp_re, xp_im, xm_re, xm_im = over_blocks(in_re_ref, in_im_ref, chan)
        hp_re, hp_im, hm_re, hm_im = over_blocks(lag_re_ref, lag_im_ref, chan)
        pp_re = xp_re * hp_re - xp_im * hp_im
        pp_im = xp_re * hp_im + xp_im * hp_re
        pm_re = xm_re * hm_re - xm_im * hm_im
        pm_im = xm_re * hm_im + xm_im * hm_re
        quarters = (pp_re + pm_re, pp_im + pm_im, pm_im - pp_im, pp_re - pm_re)
        for place, quarter in enumerate(quarters):
            rows = pl.ds((2 * chan + place // 2) * WIDTH, WIDTH)
            lanes = pl.ds(place % 2 * WIDTH, WIDTH)
            joint_hi_ref[rows, lanes], joint_lo_ref[rows, lanes] = halves(quarter)

    for chan in range(GROUP):
        joint = pl.ds(chan * SPAN, SPAN)
        rows = pl.ds(chan * BLOCKS, BLOCKS)
        sums = dot(back_ref[...], joint_hi_ref[joint, :])
        low = dot(back_ref[:BLOCKS, :], joint_lo_ref[joint, :])
        pair_hi_ref[rows, :], pair_lo_ref[rows, :] = halves(sums[:BLOCKS] + sums[BLOCKS:] + low)

    late_ref[pl.ds(0, GROUP), :] = jnp.zeros((GROUP, WIDTH), F32)
    for chan in range(GROUP):
        rows = pl.ds(chan * BLOCKS, BLOCKS)
        high, low = pair_hi_ref[rows, :], pair_lo_ref[rows, :]
        timeline = (
            dot(high, leave_hi_ref[...])
            + dot(low, leave_hi_ref[...])
            + dot(high, leave_lo_ref[...])
        )
        early_ref[pl.ds(chan, BLOCKS, stride=GROUP), :] = timeline[:, :WIDTH]
        late_ref[pl.ds(GROUP + chan, BLOCKS, stride=GROUP), :] = timeline[:, WIDTH:]
    kept_ref[...] = gain_ref[...]
    summed = early_ref[...] + late_ref[: GROUP * BLOCKS, :]
    lead = LEAD * GROUP
    out_ref[...] = jnp.concatenate(
        [
            summed[lead : lead + GROUP],
            summed[GROUP:lead],
            summed[:GROUP],
            summed[lead + GROUP :],
        ],
        axis=0,
    ).astype(BF16)


def in_vmem(value):
    return pltpu.with_memory_space_constraint(value, pltpu.VMEM)


def convolve(rows, gain, consts):
    return pl.pallas_call(
        convolve_kernel,
        out_shape=(
            pltpu.VMEM((GROUP * BLOCKS, WIDTH), BF16),
            pltpu.VMEM(gain.shape, F32),
        ),
        scratch_shapes=[
            pltpu.VMEM((GROUP * BLOCKS, WIDTH), F32),
            pltpu.VMEM((GROUP * BLOCKS, WIDTH), F32),
            pltpu.VMEM((GROUP * BLOCKS, WIDTH), F32),
            pltpu.VMEM((GROUP * BLOCKS, WIDTH), F32),
            pltpu.VMEM((GROUP * SPAN, SPAN), BF16),
            pltpu.VMEM((GROUP * SPAN, SPAN), BF16),
            pltpu.VMEM((GROUP * BLOCKS, SPAN), BF16),
            pltpu.VMEM((GROUP * BLOCKS, SPAN), BF16),
            pltpu.VMEM((GROUP * BLOCKS, WIDTH), F32),
            pltpu.VMEM((GROUP * (BLOCKS + 1), WIDTH), F32),
        ],
        name="convolve",
    )(in_vmem(rows), in_vmem(gain), *[in_vmem(table) for table in consts])


def on_device(out_gate, key_proj, value_proj, long_filter, skip_gain, residual, norm_gain):
    chans, width = key_proj.shape
    blocks = lax.axis_size("seq")
    consts = [jnp.asarray(table) for table in tables()]
    gated = lax.reduce_precision(key_proj.astype(F32) * value_proj.astype(F32), 8, 7)
    both = jnp.concatenate(
        [gated.astype(BF16).reshape(blocks, GROUP, width), long_filter.reshape(blocks, GROUP, width)],
        axis=1,
    )
    members = [led_by(LEAD, blocks)]
    arrived = lax.all_to_all(both, "seq", 0, 0, axis_index_groups=members, tiled=True)
    convolved, gain = convolve(
        arrived.reshape(2 * GROUP * blocks, width),
        norm_gain.reshape(chans // WIDTH, WIDTH),
        consts,
    )
    convolved = lax.all_to_all(
        convolved.reshape(blocks, GROUP, width),
        "seq",
        0,
        0,
        axis_index_groups=members,
        tiled=True,
    )
    convolved = convolved.reshape(chans, width).astype(F32)
    total = residual.astype(F32) + out_gate.astype(F32) * (convolved + skip_gain[:, None] * gated)
    squares = jnp.sum(total * total, axis=0, keepdims=True)
    count = lax.axis_size("ch")
    squares = jnp.sum(
        lax.all_to_all(
            jnp.broadcast_to(squares[None], (count, 1, width)),
            "ch",
            0,
            0,
            axis_index_groups=[led_by(CH_LEAD, count)],
            tiled=True,
        ),
        axis=0,
    )
    normed = total * lax.rsqrt(squares / D + 1e-06) * gain.reshape(chans)[:, None]
    return (total.astype(BF16), normed.astype(BF16))


def solution(mesh):
    return jax.shard_map(
        on_device,
        mesh=mesh,
        in_specs=(
            P("ch", "seq"),
            P("ch", "seq"),
            P("ch", "seq"),
            P("ch", "seq"),
            P("ch"),
            P("ch", "seq"),
            P("ch"),
        ),
        out_specs=(P("ch", "seq"), P("ch", "seq")),
        check_vma=False,
    )
```
